32 devices in a mesh: groups: 2 (over x), ep: 4 (over y, core), rep: 4 (over z).
Axes of the slice: x: 2, y: 2, z: 4, core: 2. Of those that a mesh axis runs over, the one named last changes fastest.
Arguments:
- prompt_hidden: bfloat16 [8, 96, 2048], P('groups', 'ep'), parts along dimension 0, may hold values from -6 to 6
- decode_hidden: bfloat16 [64, 8, 2048], P(('groups', 'ep'), 'rep'), parts along dimension 0, may hold values from -6 to 6
- queries: bfloat16 [64, 8, 2048], P(('groups', 'ep'), None, 'rep'), parts along dimension 0, may hold values from -128 to 128
- attn_gain: float32 [2048], replicated, may hold values from 0.1 to 1.9
- key_value_weight: bfloat16 [2048, 1024], P(None, 'rep'), may hold values from -0.125 to 0.125
- out_weight: bfloat16 [2048, 2048], P('rep'), may hold values from -0.5 to 0.5
- moe_gain: float32 [2048], replicated, may hold values from 0.1 to 1.9
- gate_weight: bfloat16 [16, 2048, 768], P(('ep', 'rep')), may hold values from -0.125 to 0.125
- up_weight: bfloat16 [16, 2048, 768], P(('ep', 'rep')), may hold values from -0.125 to 0.125
- down_weight: bfloat16 [16, 768, 2048], P(('ep', 'rep')), may hold values from -0.21875 to 0.21875
- expert_table: int32 [151936], replicated, may hold values from 0 to 15, as said below
- token_ids: int32 [32, 8], P('ep', 'rep'), may hold values from 0 to 151935, as said below
- prompt_lengths: int32 [8], P('groups'), parts along dimension 0, may hold values from 1 to 96, 240 in all
Outputs:
- layer_out: bfloat16 [64, 8, 2048], P(('groups', 'ep'), 'rep'), parts along dimension 0
The draws below stay inside these ranges and needn't reach their ends.
There are 2 independent parts, one for each index of `groups`. The reference program is written for one: setup_inputs(seed, part) draws one part's arguments, and reference() takes and returns one part's arrays. A program takes and returns all parts, laid end to end along the dimension named above; an argument that names none is the same for every part. Nothing has to cross between parts.
Inputs may be any that keep to these rules, and one draw needn't show every extreme that they name: `expert_table`: each expert is the value of exactly 9496 entries. `token_ids`: a device holds the 8 sequences of its index of ep at 8 // 4 steps of its index of rep; of these tokens at most 2 go to one expert; in every draw one expert receives exactly 2 from every device. `prompt_lengths`: the lengths of a group sum to 240 and the longest is 96.
All inputs are finite; a program needn't handle non-finite values.
Results may differ from the reference program's by a relative error of at most 0.017.
The reference program's roundings to bfloat16 on the way count: a program that leaves them out, or rounds other values in their place, can miss the bound.
Values may be sent and summed in bfloat16 or wider, within the bound.
A program may use at most 128 MiB of HBM per device.

```python
import math
import jax
import jax.numpy as jnp
import numpy as np
from jax import lax

MODEL_DIM = 2048
FF = 768
HEAD_DIM = 128
QUERY_HEADS = 16
KEY_VALUE_HEADS = 4
VOCAB = 151936
GROUP_PROMPTS = 4
PLEN = 96
DECODE_COUNT = 8
CAP = 2
SEQ_DEV = 8
SEQS = 32
EXPERTS = 16
N_EP = 4
N_REP = 4


def hash_order(key):
    return jax.random.permutation(jax.random.fold_in(key, 7), VOCAB).astype(jnp.int32)


def draw_expert_table(key, part):
    return (hash_order(key) % EXPERTS).astype(jnp.int32)


def draw_token_ids(key, part):
    hash_perm = hash_order(key)
    inverse = jnp.zeros((VOCAB,), jnp.int32).at[hash_perm].set(jnp.arange(VOCAB, dtype=jnp.int32))
    ep_count = SEQS // SEQ_DEV
    rep_count = EXPERTS // ep_count
    step_rows = DECODE_COUNT // rep_count
    row_count = SEQ_DEV * step_rows
    blocks = EXPERTS
    slot_cols = EXPERTS * CAP
    key_hot, key_pick, key_place, key_token = jax.random.split(jax.random.fold_in(key, 13), 4)
    hot_expert = jax.random.randint(key_hot, (), 0, EXPERTS, dtype=jnp.int32)
    columns = jnp.arange(slot_cols, dtype=jnp.int32)
    column_expert = (columns // CAP).astype(jnp.int32)
    scores = jax.random.randint(key_pick, (blocks, slot_cols), 0, 1 << 20, dtype=jnp.int32) * slot_cols + columns[None, :]
    scores = jnp.where(column_expert[None, :] == hot_expert, 1 << 30, scores)
    picked_cols = lax.top_k(scores, row_count)[1].astype(jnp.int32)
    experts = jnp.take(column_expert, picked_cols)
    place_score = jax.random.randint(key_place, (blocks, row_count), 0, 1 << 20, dtype=jnp.int32) * row_count + jnp.arange(row_count, dtype=jnp.int32)[None, :]
    row_order = jnp.argsort(place_score, axis=1).astype(jnp.int32)
    experts = jnp.take_along_axis(experts, row_order, axis=1)
    within = jax.random.randint(key_token, (blocks, row_count), 0, VOCAB // EXPERTS, dtype=jnp.int32)
    token_rows = jnp.take(inverse, experts + EXPERTS * within)
    token_rows = token_rows.reshape(ep_count, rep_count, SEQ_DEV, step_rows).transpose(0, 2, 1, 3)
    return token_rows.reshape(SEQS, DECODE_COUNT).astype(jnp.int32)


def draw_queries(key, part):
    base_draw = jnp.clip(jax.random.normal(key, (SEQS, DECODE_COUNT, QUERY_HEADS, HEAD_DIM), jnp.float32), -4.0, 4.0)
    return base_draw.reshape(SEQS, DECODE_COUNT, QUERY_HEADS * HEAD_DIM).astype(jnp.bfloat16)


def levels(own_key, dims, cuts, low, top_value):
    def one(position, shards_of):
        steps = jax.random.uniform(jax.random.fold_in(jax.random.fold_in(own_key, 6), position), (shards_of,), jnp.float32, low / len(cuts), top_value / len(cuts))
        return jnp.repeat(jnp.exp(steps), dims[position] // shards_of).reshape((-1,) + (1,) * (len(dims) - position - 1))

    gain = one(*cuts[0])
    for cut in cuts[1:]:
        gain = gain * one(*cut)
    return gain


def profile(count, total, bound, skew):
    loads = [(1 << 20) // math.isqrt(standing ** skew) + 1 for standing in range(2, count + 1)]
    spare, holding = total - bound - (count - 1), [1] * (count - 1)
    while spare > 0:
        movable = [i for i in range(count - 1) if holding[i] < bound]
        whole, left = sum([loads[i] for i in movable]), spare
        for i in movable:
            addition = min(bound - holding[i], max(1, left * loads[i] // whole), spare)
            holding[i] = holding[i] + addition
            spare = spare - addition
    return np.array([bound] + holding)


def uneven_parts(rng, count, total, reach, skew):
    if count == 2:
        one = jax.random.randint(rng, (), max(1, total - reach), min(reach, total - 1) + 1)
        return jnp.stack([one, total - one])
    sizes = jnp.asarray(profile(count, total, reach, skew), jnp.int32)
    couples = (count - 1) // 2
    donor, sink = sizes[1:1 + 2 * couples:2], sizes[2:2 + 2 * couples:2]
    margin = jnp.minimum(donor - 1, reach - sink)
    moved = jax.random.randint(jax.random.fold_in(rng, 1), (couples,), 0, 1 << 20) % (margin + 1)
    sizes = sizes.at[1:1 + 2 * couples:2].set(donor - moved).at[2:2 + 2 * couples:2].set(sink + moved)
    return sizes[jax.random.permutation(jax.random.fold_in(rng, 2), count)]


def bell_draw(own_key, shape, deviation, reach, cuts=(), kind=jnp.bfloat16):
    gain = levels(own_key, shape, cuts, -0.22, 0.18) if cuts else 1.0
    values = jax.random.normal(own_key, shape, jnp.float32) * deviation * gain
    return jnp.minimum(jnp.maximum(values, -reach), reach).astype(kind)


def setup_inputs(seed: int = 0, part: int = 0) -> dict:
    key_of = jax.random.split(jax.random.key(seed), 14)
    part_splits = jax.random.split(jax.random.fold_in(key_of[13], part), 14)
    prompt_hidden = bell_draw(part_splits[0], (GROUP_PROMPTS, PLEN, MODEL_DIM), 1.0, 6.0, ((1, 4),))
    decode_hidden = bell_draw(part_splits[1], (SEQS, DECODE_COUNT, MODEL_DIM), 1.0, 6.0, ((0, 4), (1, 4)))
    queries = draw_queries(jax.random.fold_in(jax.random.fold_in(key_of[13], part), 71), part)
    attn_gain = jnp.clip(1.0 + 0.18 * jax.random.normal(key_of[3], (MODEL_DIM,), jnp.float32), 0.1, 1.9)
    key_value_weight = bell_draw(key_of[4], (MODEL_DIM, KEY_VALUE_HEADS * 2 * HEAD_DIM), MODEL_DIM ** -0.5, 0.125, ((1, 4),))
    out_weight = bell_draw(key_of[5], (QUERY_HEADS * HEAD_DIM, MODEL_DIM), (QUERY_HEADS * HEAD_DIM // 16) ** -0.5, 0.5, ((0, 4),))
    moe_gain = jnp.clip(1.0 + 0.18 * jax.random.normal(key_of[6], (MODEL_DIM,), jnp.float32), 0.1, 1.9)
    gate_weight = bell_draw(key_of[7], (EXPERTS, MODEL_DIM, FF), MODEL_DIM ** -0.5, 0.125, ((0, 16),))
    up_weight = bell_draw(key_of[8], (EXPERTS, MODEL_DIM, FF), MODEL_DIM ** -0.5, 0.125, ((0, 16),))
    down_weight = bell_draw(key_of[9], (EXPERTS, FF, MODEL_DIM), FF ** -0.5, 0.21875, ((0, 16),))
    expert_table = draw_expert_table(jax.random.fold_in(key_of[13], 71), part)
    token_ids = draw_token_ids(jax.random.fold_in(key_of[13], 71), part)
    prompt_lengths = uneven_parts(part_splits[12], GROUP_PROMPTS, 5 * PLEN // 2, PLEN, 1).astype(jnp.int32)
    return dict(prompt_hidden=prompt_hidden, decode_hidden=decode_hidden, queries=queries, attn_gain=attn_gain, key_value_weight=key_value_weight, out_weight=out_weight, moe_gain=moe_gain, gate_weight=gate_weight, up_weight=up_weight, down_weight=down_weight, expert_table=expert_table, token_ids=token_ids, prompt_lengths=prompt_lengths)


EPS = 1e-06
THETA = 1000000.0

def rms_scale(hidden, gain_vec):
    widened = hidden.astype(jnp.float32)
    mean_sq = lax.optimization_barrier(jnp.mean(widened * widened, axis=-1, keepdims=True))
    return widened * lax.rsqrt(mean_sq + EPS) * gain_vec

def rotate(vectors, positions):
    half_dim = vectors.shape[-1] // 2
    inverse_freq = jnp.exp(jnp.arange(half_dim, dtype=jnp.float32) * (-2.0 * math.log(THETA) / vectors.shape[-1]))
    angles = positions[..., None] * inverse_freq
    cosine = jnp.cos(angles)
    sine_part = jnp.sin(angles)
    first_half = vectors[..., :half_dim]
    second_half = vectors[..., half_dim:]
    return jnp.concatenate([first_half * cosine - second_half * sine_part, second_half * cosine + first_half * sine_part], axis=-1)

def project_kv(hidden, gain_vec, key_value_weight, positions):
    leading = hidden.shape[:-1]
    normed = rms_scale(hidden, gain_vec).astype(jnp.bfloat16)
    kv_pairs = jnp.dot(normed.reshape(-1, hidden.shape[-1]), key_value_weight, preferred_element_type=jnp.float32)
    kv_pairs = kv_pairs.reshape(leading + (key_value_weight.shape[1] // (2 * HEAD_DIM), 2, HEAD_DIM))
    key_part = rotate(kv_pairs[..., 0, :], positions[..., None]).astype(jnp.bfloat16)
    value_part = kv_pairs[..., 1, :].astype(jnp.bfloat16)
    return (key_part, value_part)

def reference(prompt_hidden, decode_hidden, queries, attn_gain, key_value_weight, out_weight, moe_gain, gate_weight, up_weight, down_weight, expert_table, token_ids, prompt_lengths):
    samples = SEQS // GROUP_PROMPTS
    prompt_pos = jnp.broadcast_to(jnp.arange(PLEN, dtype=jnp.float32)[None, :], (GROUP_PROMPTS, PLEN))
    prompt_keys, prompt_values = project_kv(prompt_hidden, attn_gain, key_value_weight, prompt_pos)
    prompt_of = (jnp.arange(SEQS, dtype=jnp.int32) // samples).astype(jnp.int32)
    lengths = jnp.take(prompt_lengths, prompt_of)
    decode_pos = lengths[:, None].astype(jnp.float32) + jnp.arange(DECODE_COUNT, dtype=jnp.float32)[None, :]
    decode_keys, decode_values = project_kv(decode_hidden, attn_gain, key_value_weight, decode_pos)
    group_count = QUERY_HEADS // KEY_VALUE_HEADS
    score_scale = HEAD_DIM ** (-0.5)
    key_pos = jnp.arange(PLEN, dtype=jnp.int32)
    causal = jnp.arange(DECODE_COUNT)[None, :] <= jnp.arange(DECODE_COUNT)[:, None]
    self_mask = causal[:, None, None, :]

    def attend(sequence_index):
        query_matrix = queries[sequence_index].astype(jnp.float32).reshape(DECODE_COUNT, KEY_VALUE_HEADS, group_count, HEAD_DIM)
        prompt = prompt_of[sequence_index]
        cache_keys = prompt_keys[prompt].astype(jnp.float32)
        cache_values = prompt_values[prompt].astype(jnp.float32)
        key_valid = key_pos < lengths[sequence_index]
        cache_scores = jnp.einsum('tkgd,nkd->tkgn', query_matrix, cache_keys) * score_scale
        self_scores = jnp.einsum('tkgd,ukd->tkgu', query_matrix, decode_keys[sequence_index].astype(jnp.float32)) * score_scale
        cache_scores = jnp.where(key_valid, cache_scores, -1e+30)
        self_scores = jnp.where(self_mask, self_scores, -1e+30)
        row_top = jnp.maximum(lax.optimization_barrier(jnp.max(cache_scores, axis=-1)), lax.optimization_barrier(jnp.max(self_scores, axis=-1)))
        cache_weights = jnp.where(key_valid, jnp.exp(cache_scores - row_top[..., None]), 0.0)
        self_weights = jnp.where(self_mask, jnp.exp(self_scores - row_top[..., None]), 0.0)
        row_total = lax.optimization_barrier(jnp.sum(cache_weights, axis=-1)) + lax.optimization_barrier(jnp.sum(self_weights, axis=-1))
        numerator = jnp.einsum('tkgn,nkd->tkgd', cache_weights.astype(jnp.bfloat16).astype(jnp.float32), cache_values)
        numerator = numerator + jnp.einsum('tkgu,ukd->tkgd', self_weights.astype(jnp.bfloat16).astype(jnp.float32), decode_values[sequence_index].astype(jnp.float32))
        return (numerator / row_total[..., None]).reshape(DECODE_COUNT, QUERY_HEADS * HEAD_DIM).astype(jnp.bfloat16)
    attended = lax.map(attend, jnp.arange(SEQS, dtype=jnp.int32))
    projected = jnp.dot(attended.reshape(SEQS * DECODE_COUNT, QUERY_HEADS * HEAD_DIM), out_weight, preferred_element_type=jnp.float32).reshape(SEQS, DECODE_COUNT, MODEL_DIM)
    attn_mixed = (decode_hidden.astype(jnp.float32) + projected).astype(jnp.bfloat16)
    normed = rms_scale(attn_mixed, moe_gain).astype(jnp.bfloat16).reshape(SEQS * DECODE_COUNT, MODEL_DIM)
    chosen = jnp.take(expert_table, token_ids.reshape(-1)).astype(jnp.int32)
    row_total_count = SEQS * DECODE_COUNT
    per_expert = CAP * N_EP * N_REP

    def run_expert(collected, expert):
        row_index = jnp.nonzero(chosen == expert, size=per_expert, fill_value=row_total_count)[0].astype(jnp.int32)
        token_rows = jnp.take(normed, row_index, axis=0, mode='fill', fill_value=0)
        gate_proj = jnp.dot(token_rows, gate_weight[expert], preferred_element_type=jnp.float32)
        up_proj = jnp.dot(token_rows, up_weight[expert], preferred_element_type=jnp.float32)
        hidden = (jax.nn.silu(gate_proj) * up_proj).astype(jnp.bfloat16)
        result = jnp.dot(hidden, down_weight[expert], preferred_element_type=jnp.float32).astype(jnp.bfloat16)
        return (collected.at[row_index].set(result, mode='drop'), None)
    expert_out, unused = lax.scan(run_expert, jnp.zeros((row_total_count, MODEL_DIM), jnp.bfloat16), jnp.arange(EXPERTS, dtype=jnp.int32))
    layer_out = (attn_mixed.astype(jnp.float32) + expert_out.astype(jnp.float32).reshape(SEQS, DECODE_COUNT, MODEL_DIM)).astype(jnp.bfloat16)
    return layer_out
```

```python
import math

import functools

import jax
import jax.numpy as jnp
import numpy as np
from jax import lax
from jax.experimental import pallas as pl
from jax.experimental.pallas import tpu as pltpu
from jax.sharding import PartitionSpec as P

HEAD_DIM = 128
QUERY_HEADS = 16
KEY_VALUE_HEADS = 4
GROUP_PROMPTS = 4
CAP = 2


EPS = 1e-06
THETA = 1000000.0


def swapped(block, axis, bit):
    count = lax.axis_size(axis)
    route = []
    for low in range(count):
        high = low | 1 << bit
        if high != low and high < count:
            route += [(low, high), (high, low)]
    return lax.ppermute(block, axis, route)


def rms_scale(hidden, gain_vec):
    widened = hidden.astype(jnp.float32)
    mean_sq = jnp.mean(widened * widened, axis=-1, keepdims=True)
    return widened * lax.rsqrt(mean_sq + EPS) * gain_vec


def rotate(vectors, positions):
    half_dim = vectors.shape[-1] // 2
    inverse_freq = jnp.exp(
        jnp.arange(half_dim, dtype=jnp.float32) * (-2.0 * math.log(THETA) / vectors.shape[-1])
    )
    angles = positions[..., None] * inverse_freq
    cosine = jnp.cos(angles)
    sine_part = jnp.sin(angles)
    first_half = vectors[..., :half_dim]
    second_half = vectors[..., half_dim:]
    return jnp.concatenate(
        [
            first_half * cosine - second_half * sine_part,
            second_half * cosine + first_half * sine_part,
        ],
        axis=-1,
    )


def expert_apply(tokens, gate_weight, up_weight, down_weight):
    flat_rows = tokens.reshape(-1, tokens.shape[-1])
    gate_proj = jnp.dot(flat_rows, gate_weight[0], preferred_element_type=jnp.float32)
    up_proj = jnp.dot(flat_rows, up_weight[0], preferred_element_type=jnp.float32)
    hidden = (jax.nn.silu(gate_proj) * up_proj).astype(jnp.bfloat16)
    return (
        jnp.dot(hidden, down_weight[0], preferred_element_type=jnp.float32)
        .astype(jnp.bfloat16)
        .reshape(tokens.shape)
    )


def local(
    prompt_hidden,
    decode_hidden,
    queries,
    attn_gain,
    key_value_weight,
    out_weight,
    moe_gain,
    gate_weight,
    up_weight,
    down_weight,
    expert_table,
    token_ids,
    prompt_lengths,
):
    full_hidden = lax.all_gather(decode_hidden, "rep", axis=1, tiled=True)
    sequences_local, steps_total, model_width = full_hidden.shape
    prompt_length_local = prompt_hidden.shape[1]
    qh_dev = queries.shape[2] // HEAD_DIM
    group_count = QUERY_HEADS // KEY_VALUE_HEADS
    ep_count = lax.axis_size("ep")
    rep_count = lax.axis_size("rep")
    ep_index = lax.axis_index("ep")
    rep_index = lax.axis_index("rep")
    seq_total = sequences_local * ep_count
    samples = seq_total // GROUP_PROMPTS
    score_scale = HEAD_DIM ** (-0.5)
    step_rows = steps_total // rep_count
    blocks = key_value_weight.shape[1] // HEAD_DIM

    def own_columns(hidden, positions):
        leading = hidden.shape[:-1]
        normed = rms_scale(hidden, attn_gain).astype(jnp.bfloat16)
        projected = jnp.dot(
            normed.reshape(-1, model_width), key_value_weight, preferred_element_type=jnp.float32
        )
        projected = projected.reshape(leading + (blocks, HEAD_DIM))
        block_ids = rep_index * blocks + jnp.arange(blocks, dtype=jnp.int32)
        is_key = (block_ids % 2 == 0)[:, None]
        turned = rotate(projected, positions[..., None])
        return (
            jnp.where(is_key, turned, projected)
            .astype(jnp.bfloat16)
            .reshape(leading + (blocks * HEAD_DIM,))
        )

    key_pos = ep_index * prompt_length_local + jnp.arange(prompt_length_local, dtype=jnp.int32)
    prompt_pos = jnp.broadcast_to(
        key_pos.astype(jnp.float32)[None, :], (GROUP_PROMPTS, prompt_length_local)
    )
    own_seqs = ep_index * sequences_local + jnp.arange(sequences_local, dtype=jnp.int32)
    own_prompt = own_seqs // samples
    own_lengths = jnp.take(prompt_lengths, own_prompt)
    decode_pos = (
        own_lengths[:, None].astype(jnp.float32)
        + jnp.arange(steps_total, dtype=jnp.float32)[None, :]
    )
    prompt_part = own_columns(prompt_hidden, prompt_pos)
    decode_part = own_columns(full_hidden, decode_pos)
    prompt_hot = own_prompt[:, None] == jnp.arange(GROUP_PROMPTS, dtype=jnp.int32)[None, :]
    if blocks == 1:
        partner_prompt, partner_decode = swapped((prompt_part, decode_part), "rep", 0)
        holds_key = rep_index % 2 == 0
        prompt_columns = jnp.where(
            holds_key,
            jnp.concatenate([prompt_part, partner_prompt], axis=2),
            jnp.concatenate([partner_prompt, prompt_part], axis=2),
        )
        decode_columns = jnp.where(
            holds_key,
            jnp.concatenate([decode_part, partner_decode], axis=2),
            jnp.concatenate([partner_decode, decode_part], axis=2),
        )
        heads_here = 1
        head_base = rep_index // 2
    else:
        prompt_columns = prompt_part
        decode_columns = decode_part
        heads_here = blocks // 2
        head_base = rep_index * heads_here
    prompt_key_value = prompt_columns.reshape(
        GROUP_PROMPTS, prompt_length_local, heads_here, 2, HEAD_DIM
    )
    decode_key_value = decode_columns.reshape(sequences_local, steps_total, heads_here, 2, HEAD_DIM)
    prompt_keys = prompt_key_value[:, :, :, 0, :]
    prompt_values = prompt_key_value[:, :, :, 1, :]
    decode_keys = decode_key_value[:, :, :, 0, :]
    decode_values = decode_key_value[:, :, :, 1, :]
    query_matrix = queries.reshape(sequences_local, steps_total, qh_dev, HEAD_DIM)
    head_pick = (
        rep_index * qh_dev + jnp.arange(qh_dev, dtype=jnp.int32)
    ) // group_count - head_base
    own_keys = jnp.take(decode_keys, head_pick, axis=2)
    own_values = jnp.take(decode_values, head_pick, axis=2)
    self_scores = (
        jnp.einsum("sthd,suhd->sthu", query_matrix, own_keys, preferred_element_type=jnp.float32)
        * score_scale
    )
    self_mask = (
        jnp.arange(steps_total, dtype=jnp.int32)[None, :]
        <= jnp.arange(steps_total, dtype=jnp.int32)[:, None]
    )[None, :, None, :]
    self_scores = jnp.where(self_mask, self_scores, -1e30)
    self_top = jnp.max(self_scores, axis=-1)
    start_weights = jnp.where(self_mask, jnp.exp(self_scores - self_top[..., None]), 0.0)
    row_top = self_top
    row_total = jnp.sum(start_weights, axis=-1)
    weighted = jnp.einsum(
        "sthu,suhd->sthd",
        start_weights.astype(jnp.bfloat16),
        own_values,
        preferred_element_type=jnp.float32,
    )
    piece_keys = jnp.take(lax.all_gather(prompt_keys, "ep", axis=1, tiled=True), head_pick, axis=2)
    piece_values = jnp.take(
        lax.all_gather(prompt_values, "ep", axis=1, tiled=True), head_pick, axis=2
    )
    piece_len = piece_keys.shape[1]
    valid = jnp.arange(piece_len, dtype=jnp.int32)[None, :] < prompt_lengths[:, None]
    key_mask = prompt_hot[:, None, None, :, None] & valid[None, None, None, :, :]
    scores = (
        jnp.einsum("sthd,pnhd->sthpn", query_matrix, piece_keys, preferred_element_type=jnp.float32)
        * score_scale
    )
    scores = jnp.where(key_mask, scores, -1e30)
    new_top = jnp.maximum(row_top, jnp.max(scores, axis=(-2, -1)))
    decay = jnp.exp(row_top - new_top)
    weights = jnp.where(key_mask, jnp.exp(scores - new_top[..., None, None]), 0.0)
    weighted = weighted * decay[..., None] + jnp.einsum(
        "sthpn,pnhd->sthd",
        weights.astype(jnp.bfloat16),
        piece_values,
        preferred_element_type=jnp.float32,
    )
    row_top, row_total, weighted = (
        new_top,
        row_total * decay + jnp.sum(weights, axis=(-2, -1)),
        weighted,
    )
    attended = weighted / row_total[..., None]
    heads_out = attended.reshape(sequences_local, steps_total, qh_dev * HEAD_DIM).astype(
        jnp.bfloat16
    )
    by_step = jnp.swapaxes(heads_out, 0, 1)
    attn_sum = jnp.swapaxes(
        lax.psum_scatter(
            jnp.dot(
                by_step.reshape(-1, by_step.shape[-1]),
                out_weight,
                preferred_element_type=jnp.float32,
            )
            .reshape(step_rows * lax.axis_size("rep"), sequences_local, model_width)
            .astype(jnp.bfloat16),
            "rep",
            scatter_dimension=0,
            tiled=True,
        ).astype(jnp.float32),
        0,
        1,
    )
    attn_mixed = (decode_hidden.astype(jnp.float32) + attn_sum).astype(jnp.bfloat16)
    row_count = sequences_local * step_rows
    normed = rms_scale(attn_mixed, moe_gain).astype(jnp.bfloat16).reshape(row_count, model_width)
    chosen = jnp.take(expert_table, token_ids.reshape(row_count))
    device_count = ep_count * rep_count
    slot_total = device_count * CAP
    same_expert = chosen[:, None] == chosen[None, :]
    before = jnp.arange(row_count)[None, :] < jnp.arange(row_count)[:, None]
    slot_rank = jnp.sum((same_expert & before).astype(jnp.int32), axis=1)
    destination = chosen * CAP + slot_rank
    send_pick = (jnp.arange(slot_total, dtype=jnp.int32)[:, None] == destination[None, :]).astype(
        jnp.bfloat16
    )
    outgoing = (
        jnp.dot(send_pick, normed, preferred_element_type=jnp.float32)
        .astype(jnp.bfloat16)
        .reshape(device_count, CAP, model_width)
    )
    served = expert_apply(
        lax.all_to_all(outgoing, ("ep", "rep"), split_axis=0, concat_axis=0, tiled=True),
        gate_weight,
        up_weight,
        down_weight,
    )
    returned = lax.all_to_all(served, ("ep", "rep"), split_axis=0, concat_axis=0, tiled=True)
    moe_out = lax.dot_general(
        send_pick,
        returned.reshape(slot_total, model_width),
        (((0,), (0,)), ((), ())),
        preferred_element_type=jnp.float32,
    )
    layer_out = (
        attn_mixed.astype(jnp.float32) + moe_out.reshape(sequences_local, step_rows, model_width)
    ).astype(jnp.bfloat16)
    return layer_out


BF = jnp.bfloat16
F32 = jnp.float32
MESH = pl.DeviceIdType.MESH
KEY_PAD = 32


def rotary_table(count):
    half = HEAD_DIM // 2
    freq = THETA ** (-2.0 * np.arange(half) / HEAD_DIM)
    angle = np.arange(count)[:, None] * freq[None, :]
    cosine, sine = np.cos(angle), np.sin(angle)
    return np.concatenate([cosine, cosine, -sine, sine], axis=1).astype(np.float32)


def iota(shape, dim):
    return lax.broadcasted_iota(jnp.int32, shape, dim)


def turned(vectors, positions, table):
    count = table.shape[0]
    hot = (iota((positions.shape[0], count), 1) == positions).astype(F32)
    both = jnp.dot(hot, table, precision=lax.Precision.HIGHEST, preferred_element_type=F32)
    return vectors * both[:, :HEAD_DIM] + pltpu.roll(vectors, HEAD_DIM // 2, 1) * both[:, HEAD_DIM:]


def fused_kernel(
    dims,
    tok, lens, rot, ph, dh, q, again, kvw, ow, mgain, gw, uw, dw, table,
    out,
    rot_v, ph_v, hid, q_v, again_v, kvw_v, ow_v, mgain_v, gw_v, uw_v, dw_v, table_v,
    picked, kv_send, kv_land, part_send, part_land, tok_send, tok_land, ret_send, ret_land,
    load_sem, hid_s, hid_r, kv_s, kv_r, part_s, part_r, tok_s, tok_r, ret_s, ret_r, own_sem,
):
    ep_n, rep_n, seqs, steps, chunk, step_rows = dims
    ep = lax.axis_index("ep")
    rep = lax.axis_index("rep")
    devices = ep_n * rep_n
    me = ep * rep_n + rep
    rows = seqs * step_rows
    total_rows = rows * rep_n
    qh = q.shape[1] // HEAD_DIM

    def flat(k):
        other = lax.rem(me + k, devices)
        return {"ep": lax.div(other, rep_n), "rep": lax.rem(other, rep_n)}

    loads = {}
    for n, (name, a, b) in enumerate([
        ("dh", dh, hid.at[rep]), ("ph", ph, ph_v), ("again", again, again_v), ("kvw", kvw, kvw_v),
        ("rot", rot, rot_v), ("q", q, q_v), ("table", table, table_v), ("ow", ow, ow_v),
        ("mgain", mgain, mgain_v), ("gw", gw, gw_v), ("uw", uw, uw_v), ("dw", dw, dw_v),
    ]):
        loads[name] = pltpu.make_async_copy(a, b, load_sem.at[n])
        loads[name].start()

    barrier = pltpu.get_barrier_semaphore()
    for k in range(1, devices):
        pl.semaphore_signal(barrier, inc=1, device_id=flat(k), device_id_type=MESH)
    pl.semaphore_wait(barrier, devices - 1)

    loads["dh"].wait()
    hid_copies = []
    for k in range(1, rep_n):
        peer = lax.rem(rep + k, rep_n)
        c = pltpu.make_async_remote_copy(
            src_ref=hid.at[rep], dst_ref=hid.at[rep], send_sem=hid_s.at[k], recv_sem=hid_r.at[k],
            device_id={"rep": peer}, device_id_type=MESH)
        c.start()
        hid_copies.append(c)

    def normed(values, gain):
        wide = values.astype(F32)
        mean_sq = jnp.mean(wide * wide, axis=-1, keepdims=True)
        return (wide * lax.rsqrt(mean_sq + EPS) * gain).astype(BF)

    for name in ("ph", "again", "kvw", "rot"):
        loads[name].wait()
    rot_t = rot_v[...]
    prompts = ph.shape[0] // chunk
    proj = jnp.dot(normed(ph_v[...], again_v[...]), kvw_v[...], preferred_element_type=F32)
    pos = ep * chunk + lax.rem(iota((prompts * chunk, 1), 0), chunk)
    keys = turned(proj[:, :HEAD_DIM], pos, rot_t)
    pad = jnp.zeros((KEY_PAD - chunk, HEAD_DIM), F32)
    for p in range(prompts):
        cut = slice(p * chunk, (p + 1) * chunk)
        kv_send[p, :, :HEAD_DIM] = jnp.concatenate([keys[cut], pad], axis=0).astype(BF)
        kv_send[p, :, HEAD_DIM:] = jnp.concatenate([proj[cut, HEAD_DIM:], pad], axis=0).astype(BF)
    kv_copies = []
    for k in range(1, ep_n):
        peer = lax.rem(ep + k, ep_n)
        c = pltpu.make_async_remote_copy(
            src_ref=kv_send.at[peer], dst_ref=kv_land.at[ep], send_sem=kv_s.at[k], recv_sem=kv_r.at[k],
            device_id={"ep": peer}, device_id_type=MESH)
        c.start()
        kv_copies.append(c)
    kv_own = pltpu.make_async_copy(kv_send.at[ep], kv_land.at[ep], own_sem.at[0])
    kv_own.start()

    loads["q"].wait()
    r0 = iota((total_rows, 1), 0)
    seq0 = lax.div(lax.rem(r0, rows), step_rows)
    step0 = lax.div(r0, rows) * step_rows + lax.rem(r0, step_rows)
    perm = (iota((total_rows, total_rows), 1) == seq0 * steps + step0).astype(BF)
    q_perm = jnp.dot(perm, q_v[...], preferred_element_type=F32)
    q_cat = jnp.concatenate(
        [q_perm[:, h * HEAD_DIM:(h + 1) * HEAD_DIM] for h in range(qh)], axis=0).astype(BF)

    loads["table"].wait()
    i0 = iota((rows, 1), 0)
    lane = jnp.zeros((rows, 1), jnp.int32)
    for i in range(rows):
        t = tok[i]
        picked[pl.ds(i, 1), :] = table_v[pl.ds(lax.shift_right_logical(t, 7), 1), :]
        lane = jnp.where(i0 == i, t & 127, lane)
    got = picked[...].astype(F32)
    chosen_c = jnp.sum(jnp.where(iota(got.shape, 1) == lane, got, 0.0), axis=1, keepdims=True)
    a_i, b_i = iota((rows, rows), 0), iota((rows, rows), 1)
    chosen_r = jnp.sum(jnp.where(a_i == b_i, chosen_c, 0.0), axis=0, keepdims=True)
    same = chosen_c == chosen_r
    rank_c = jnp.sum(jnp.where(same & (b_i < a_i), 1.0, 0.0), axis=1, keepdims=True)
    rank_r = jnp.sum(jnp.where(same & (a_i < b_i), 1.0, 0.0), axis=0, keepdims=True)
    slots = devices * CAP
    dest_r = (chosen_r * CAP + rank_r).astype(jnp.int32)
    dest_c = (chosen_c * CAP + rank_c).astype(jnp.int32)
    pick = (iota((slots, rows), 0) == dest_r).astype(BF)
    unpick = (iota((rows, slots), 1) == dest_c).astype(BF)

    length = lens[ep]
    keys_p = ep_n * KEY_PAD
    n_keys = keys_p + total_rows
    qr = lax.rem(iota((qh * total_rows, 1), 0), total_rows)
    q_seq = lax.div(lax.rem(qr, rows), step_rows)
    q_step = lax.div(qr, rows) * step_rows + lax.rem(qr, step_rows)
    kc = iota((1, n_keys), 1)
    inner = lax.rem(kc, KEY_PAD)
    p_ok = (kc < keys_p) & (inner < chunk) & (lax.div(kc, KEY_PAD) * chunk + inner < length)
    kr = jnp.maximum(kc - keys_p, 0)
    k_seq = jnp.where(kc < keys_p, -1, lax.div(lax.rem(kr, rows), step_rows))
    k_step = jnp.where(p_ok, -1, lax.div(kr, rows) * step_rows + lax.rem(kr, step_rows))
    k_seq_p = jnp.where(p_ok, 1, 0)
    mask = ((q_seq == k_seq) | (k_seq_p == 1)) & (k_step <= q_step)

    for c in hid_copies:
        c.wait_recv()
    hidden = hid[...].reshape(total_rows, hid.shape[2])
    proj_d = jnp.dot(normed(hidden, again_v[...]), kvw_v[...], preferred_element_type=F32)
    keys_d = turned(proj_d[:, :HEAD_DIM], length + step0, rot_t).astype(BF)
    vals_d = proj_d[:, HEAD_DIM:].astype(BF)
    for c in kv_copies:
        c.wait_recv()
    kv_own.wait()
    kv_all = kv_land[...].reshape(keys_p, 2 * HEAD_DIM)
    k_all = jnp.concatenate([kv_all[:, :HEAD_DIM], keys_d], axis=0)
    v_all = jnp.concatenate([kv_all[:, HEAD_DIM:], vals_d], axis=0)
    scores = lax.dot_general(
        q_cat, k_all, (((1,), (1,)), ((), ())), preferred_element_type=F32) * HEAD_DIM ** (-0.5)
    scores = jnp.where(mask, scores, -1e30)
    top = jnp.max(scores, axis=-1, keepdims=True)
    weights = jnp.where(mask, jnp.exp(scores - top), 0.0)
    row_total = jnp.sum(weights, axis=-1, keepdims=True)
    att = jnp.dot(weights.astype(BF), v_all, preferred_element_type=F32) / row_total
    att = jnp.concatenate(
        [att[h * total_rows:(h + 1) * total_rows] for h in range(qh)], axis=1).astype(BF)
    loads["ow"].wait()
    part = jnp.dot(att, ow_v[...], preferred_element_type=F32).astype(BF)
    part_send[...] = part.reshape(part_send.shape)
    part_copies = []
    for k in range(1, rep_n):
        peer = lax.rem(rep + k, rep_n)
        c = pltpu.make_async_remote_copy(
            src_ref=part_send.at[peer], dst_ref=part_land.at[k - 1], send_sem=part_s.at[k],
            recv_sem=part_r.at[k], device_id={"rep": peer}, device_id_type=MESH)
        c.start()
        part_copies.append(c)
    attn_sum = part_send[rep].astype(F32)
    loads["mgain"].wait()
    for k, c in enumerate(part_copies):
        c.wait_recv()
        attn_sum = attn_sum + part_land[k].astype(F32)
    mixed = (hid[rep].astype(F32) + attn_sum).astype(BF)
    tokens = normed(mixed, mgain_v[...])

    def scatter(values, send, land, sends, recvs, own):
        for d in range(devices):
            send[d] = values[d * CAP:(d + 1) * CAP, :]
        copies = []
        for k in range(1, devices):
            other = lax.rem(me + k, devices)
            c = pltpu.make_async_remote_copy(
                src_ref=send.at[other], dst_ref=land.at[me], send_sem=sends.at[k],
                recv_sem=recvs.at[k], device_id=flat(k), device_id_type=MESH)
            c.start()
            copies.append(c)
        mine = pltpu.make_async_copy(send.at[me], land.at[me], own)
        mine.start()
        return copies, mine

    outgoing = jnp.dot(pick, tokens, preferred_element_type=F32).astype(BF)
    tok_copies, tok_own = scatter(outgoing, tok_send, tok_land, tok_s, tok_r, own_sem.at[1])
    for name in ("gw", "uw", "dw"):
        loads[name].wait()
    for c in tok_copies:
        c.wait_recv()
    tok_own.wait()
    served_in = jnp.concatenate([tok_land[d] for d in range(devices)], axis=0)
    gate = jnp.dot(served_in, gw_v[...], preferred_element_type=F32)
    up = jnp.dot(served_in, uw_v[...], preferred_element_type=F32)
    act = (gate / (1.0 + jnp.exp(-gate)) * up).astype(BF)
    served = jnp.dot(act, dw_v[...], preferred_element_type=F32).astype(BF)
    ret_copies, ret_own = scatter(served, ret_send, ret_land, ret_s, ret_r, own_sem.at[2])
    for c in ret_copies:
        c.wait_recv()
    ret_own.wait()
    back = jnp.concatenate([ret_land[d] for d in range(devices)], axis=0)
    moe = jnp.dot(unpick, back, preferred_element_type=F32)
    out[...] = (mixed.astype(F32) + moe).astype(BF)
    for c in hid_copies + kv_copies + part_copies + tok_copies + ret_copies:
        c.wait_send()


def fused_local(
    prompt_hidden, decode_hidden, queries, attn_gain, key_value_weight, out_weight, moe_gain,
    gate_weight, up_weight, down_weight, expert_table, token_ids, prompt_lengths,
):
    ep_n, rep_n = lax.axis_size("ep"), lax.axis_size("rep")
    prompts, chunk, width = prompt_hidden.shape
    seqs, step_rows, _ = decode_hidden.shape
    steps = queries.shape[1]
    ff = gate_weight.shape[2]
    devices = ep_n * rep_n
    rows = seqs * step_rows
    columns = key_value_weight.shape[1]
    count = -(-(chunk * ep_n + steps) // 128) * 128
    dims = (ep_n, rep_n, seqs, steps, chunk, step_rows)
    any_spec = pl.BlockSpec(memory_space=pl.ANY)
    smem = pl.BlockSpec(memory_space=pltpu.SMEM)
    vm = pltpu.VMEM
    dma = pltpu.SemaphoreType.DMA
    args = (
        token_ids.reshape(rows), prompt_lengths, jnp.asarray(rotary_table(count)),
        prompt_hidden.reshape(prompts * chunk, width), decode_hidden.reshape(rows, width),
        queries.reshape(seqs * steps, queries.shape[2]), attn_gain.reshape(1, width),
        key_value_weight, out_weight, moe_gain.reshape(1, width),
        gate_weight[0], up_weight[0], down_weight[0], expert_table.reshape(-1, 128),
    )
    slab = (devices, CAP, width)
    out = pl.pallas_call(
        functools.partial(fused_kernel, dims),
        out_shape=jax.ShapeDtypeStruct((rows, width), BF),
        in_specs=[smem, smem] + [any_spec] * 12,
        out_specs=pl.BlockSpec(memory_space=pltpu.VMEM),
        scratch_shapes=[
            vm((count, 2 * HEAD_DIM), F32), vm((prompts * chunk, width), BF), vm((rep_n, rows, width), BF),
            vm((seqs * steps, queries.shape[2]), BF), vm((1, width), F32), vm((width, columns), BF),
            vm(out_weight.shape, BF), vm((1, width), F32), vm((width, ff), BF), vm((width, ff), BF),
            vm((ff, width), BF), vm((expert_table.shape[0] // 128, 128), jnp.int32),
            vm((rows, 128), jnp.int32),
            vm((prompts, KEY_PAD, columns), BF), vm((ep_n, KEY_PAD, columns), BF),
            vm((rep_n, rows, width), BF), vm((rep_n - 1, rows, width), BF),
            vm(slab, BF), vm(slab, BF), vm(slab, BF), vm(slab, BF),
            dma((12,)), dma((rep_n,)), dma((rep_n,)), dma((ep_n,)), dma((ep_n,)), dma((rep_n,)),
            dma((rep_n,)), dma((devices,)), dma((devices,)), dma((devices,)), dma((devices,)), dma((3,)),
        ],
        compiler_params=pltpu.CompilerParams(
            collective_id=0, has_side_effects=True, vmem_limit_bytes=60 * 1024 * 1024),
    )(*args)
    return out.reshape(decode_hidden.shape)


def pick_local(*args):
    prompt_hidden, decode_hidden, queries, key_value_weight = args[0], args[1], args[2], args[4]
    one_prompt = (
        decode_hidden.shape[0] * lax.axis_size("ep") // GROUP_PROMPTS == decode_hidden.shape[0]
        and lax.axis_size("ep") == GROUP_PROMPTS
    )
    one_head = key_value_weight.shape[1] == 2 * HEAD_DIM
    if one_prompt and one_head and prompt_hidden.shape[1] <= KEY_PAD and prompt_hidden.shape[1] % 8 == 0:
        return fused_local(*args)
    return local(*args)


def solution(mesh):
    placed = (
        P("groups", "ep", None),
        P(("groups", "ep"), "rep", None),
        P(("groups", "ep"), None, "rep"),
        P(),
        P(None, "rep"),
        P("rep", None),
        P(),
        P(("ep", "rep"), None, None),
        P(("ep", "rep"), None, None),
        P(("ep", "rep"), None, None),
        P(),
        P("ep", "rep"),
        P("groups"),
    )
    return jax.shard_map(
        pick_local,
        mesh=mesh,
        in_specs=placed,
        out_specs=P(("groups", "ep"), "rep", None),
        check_vma=False,
    )
```

```python
import math

import functools

import jax
import jax.numpy as jnp
import numpy as np
from jax import lax
from jax.experimental import pallas as pl
from jax.experimental.pallas import tpu as pltpu
from jax.sharding import PartitionSpec as P

HEAD_DIM = 128
QUERY_HEADS = 16
KEY_VALUE_HEADS = 4
GROUP_PROMPTS = 4
CAP = 2


EPS = 1e-06
THETA = 1000000.0


def swapped(block, axis, bit):
    count = lax.axis_size(axis)
    route = []
    for low in range(count):
        high = low | 1 << bit
        if high != low and high < count:
            route += [(low, high), (high, low)]
    return lax.ppermute(block, axis, route)


def rms_scale(hidden, gain_vec):
    widened = hidden.astype(jnp.float32)
    mean_sq = jnp.mean(widened * widened, axis=-1, keepdims=True)
    return widened * lax.rsqrt(mean_sq + EPS) * gain_vec


def rotate(vectors, positions):
    half_dim = vectors.shape[-1] // 2
    inverse_freq = jnp.exp(
        jnp.arange(half_dim, dtype=jnp.float32) * (-2.0 * math.log(THETA) / vectors.shape[-1])
    )
    angles = positions[..., None] * inverse_freq
    cosine = jnp.cos(angles)
    sine_part = jnp.sin(angles)
    first_half = vectors[..., :half_dim]
    second_half = vectors[..., half_dim:]
    return jnp.concatenate(
        [
            first_half * cosine - second_half * sine_part,
            second_half * cosine + first_half * sine_part,
        ],
        axis=-1,
    )


def expert_apply(tokens, gate_weight, up_weight, down_weight):
    flat_rows = tokens.reshape(-1, tokens.shape[-1])
    gate_proj = jnp.dot(flat_rows, gate_weight[0], preferred_element_type=jnp.float32)
    up_proj = jnp.dot(flat_rows, up_weight[0], preferred_element_type=jnp.float32)
    hidden = (jax.nn.silu(gate_proj) * up_proj).astype(jnp.bfloat16)
    return (
        jnp.dot(hidden, down_weight[0], preferred_element_type=jnp.float32)
        .astype(jnp.bfloat16)
        .reshape(tokens.shape)
    )


def local(
    prompt_hidden,
    decode_hidden,
    queries,
    attn_gain,
    key_value_weight,
    out_weight,
    moe_gain,
    gate_weight,
    up_weight,
    down_weight,
    expert_table,
    token_ids,
    prompt_lengths,
):
    full_hidden = lax.all_gather(decode_hidden, "rep", axis=1, tiled=True)
    sequences_local, steps_total, model_width = full_hidden.shape
    prompt_length_local = prompt_hidden.shape[1]
    qh_dev = queries.shape[2] // HEAD_DIM
    group_count = QUERY_HEADS // KEY_VALUE_HEADS
    ep_count = lax.axis_size("ep")
    rep_count = lax.axis_size("rep")
    ep_index = lax.axis_index("ep")
    rep_index = lax.axis_index("rep")
    seq_total = sequences_local * ep_count
    samples = seq_total // GROUP_PROMPTS
    score_scale = HEAD_DIM ** (-0.5)
    step_rows = steps_total // rep_count
    blocks = key_value_weight.shape[1] // HEAD_DIM

    def own_columns(hidden, positions):
        leading = hidden.shape[:-1]
        normed = rms_scale(hidden, attn_gain).astype(jnp.bfloat16)
        projected = jnp.dot(
            normed.reshape(-1, model_width), key_value_weight, preferred_element_type=jnp.float32
        )
        projected = projected.reshape(leading + (blocks, HEAD_DIM))
        block_ids = rep_index * blocks + jnp.arange(blocks, dtype=jnp.int32)
        is_key = (block_ids % 2 == 0)[:, None]
        turned = rotate(projected, positions[..., None])
        return (
            jnp.where(is_key, turned, projected)
            .astype(jnp.bfloat16)
            .reshape(leading + (blocks * HEAD_DIM,))
        )

    key_pos = ep_index * prompt_length_local + jnp.arange(prompt_length_local, dtype=jnp.int32)
    prompt_pos = jnp.broadcast_to(
        key_pos.astype(jnp.float32)[None, :], (GROUP_PROMPTS, prompt_length_local)
    )
    own_seqs = ep_index * sequences_local + jnp.arange(sequences_local, dtype=jnp.int32)
    own_prompt = own_seqs // samples
    own_lengths = jnp.take(prompt_lengths, own_prompt)
    decode_pos = (
        own_lengths[:, None].astype(jnp.float32)
        + jnp.arange(steps_total, dtype=jnp.float32)[None, :]
    )
    prompt_part = own_columns(prompt_hidden, prompt_pos)
    decode_part = own_columns(full_hidden, decode_pos)
    prompt_hot = own_prompt[:, None] == jnp.arange(GROUP_PROMPTS, dtype=jnp.int32)[None, :]
    if blocks == 1:
        partner_prompt, partner_decode = swapped((prompt_part, decode_part), "rep", 0)
        holds_key = rep_index % 2 == 0
        prompt_columns = jnp.where(
            holds_key,
            jnp.concatenate([prompt_part, partner_prompt], axis=2),
            jnp.concatenate([partner_prompt, prompt_part], axis=2),
        )
        decode_columns = jnp.where(
            holds_key,
            jnp.concatenate([decode_part, partner_decode], axis=2),
            jnp.concatenate([partner_decode, decode_part], axis=2),
        )
        heads_here = 1
        head_base = rep_index // 2
    else:
        prompt_columns = prompt_part
        decode_columns = decode_part
        heads_here = blocks // 2
        head_base = rep_index * heads_here
    prompt_key_value = prompt_columns.reshape(
        GROUP_PROMPTS, prompt_length_local, heads_here, 2, HEAD_DIM
    )
    decode_key_value = decode_columns.reshape(sequences_local, steps_total, heads_here, 2, HEAD_DIM)
    prompt_keys = prompt_key_value[:, :, :, 0, :]
    prompt_values = prompt_key_value[:, :, :, 1, :]
    decode_keys = decode_key_value[:, :, :, 0, :]
    decode_values = decode_key_value[:, :, :, 1, :]
    query_matrix = queries.reshape(sequences_local, steps_total, qh_dev, HEAD_DIM)
    head_pick = (
        rep_index * qh_dev + jnp.arange(qh_dev, dtype=jnp.int32)
    ) // group_count - head_base
    own_keys = jnp.take(decode_keys, head_pick, axis=2)
    own_values = jnp.take(decode_values, head_pick, axis=2)
    self_scores = (
        jnp.einsum("sthd,suhd->sthu", query_matrix, own_keys, preferred_element_type=jnp.float32)
        * score_scale
    )
    self_mask = (
        jnp.arange(steps_total, dtype=jnp.int32)[None, :]
        <= jnp.arange(steps_total, dtype=jnp.int32)[:, None]
    )[None, :, None, :]
    self_scores = jnp.where(self_mask, self_scores, -1e30)
    self_top = jnp.max(self_scores, axis=-1)
    start_weights = jnp.where(self_mask, jnp.exp(self_scores - self_top[..., None]), 0.0)
    row_top = self_top
    row_total = jnp.sum(start_weights, axis=-1)
    weighted = jnp.einsum(
        "sthu,suhd->sthd",
        start_weights.astype(jnp.bfloat16),
        own_values,
        preferred_element_type=jnp.float32,
    )
    piece_keys = jnp.take(lax.all_gather(prompt_keys, "ep", axis=1, tiled=True), head_pick, axis=2)
    piece_values = jnp.take(
        lax.all_gather(prompt_values, "ep", axis=1, tiled=True), head_pick, axis=2
    )
    piece_len = piece_keys.shape[1]
    valid = jnp.arange(piece_len, dtype=jnp.int32)[None, :] < prompt_lengths[:, None]
    key_mask = prompt_hot[:, None, None, :, None] & valid[None, None, None, :, :]
    scores = (
        jnp.einsum("sthd,pnhd->sthpn", query_matrix, piece_keys, preferred_element_type=jnp.float32)
        * score_scale
    )
    scores = jnp.where(key_mask, scores, -1e30)
    new_top = jnp.maximum(row_top, jnp.max(scores, axis=(-2, -1)))
    decay = jnp.exp(row_top - new_top)
    weights = jnp.where(key_mask, jnp.exp(scores - new_top[..., None, None]), 0.0)
    weighted = weighted * decay[..., None] + jnp.einsum(
        "sthpn,pnhd->sthd",
        weights.astype(jnp.bfloat16),
        piece_values,
        preferred_element_type=jnp.float32,
    )
    row_top, row_total, weighted = (
        new_top,
        row_total * decay + jnp.sum(weights, axis=(-2, -1)),
        weighted,
    )
    attended = weighted / row_total[..., None]
    heads_out = attended.reshape(sequences_local, steps_total, qh_dev * HEAD_DIM).astype(
        jnp.bfloat16
    )
    by_step = jnp.swapaxes(heads_out, 0, 1)
    attn_sum = jnp.swapaxes(
        lax.psum_scatter(
            jnp.dot(
                by_step.reshape(-1, by_step.shape[-1]),
                out_weight,
                preferred_element_type=jnp.float32,
            )
            .reshape(step_rows * lax.axis_size("rep"), sequences_local, model_width)
            .astype(jnp.bfloat16),
            "rep",
            scatter_dimension=0,
            tiled=True,
        ).astype(jnp.float32),
        0,
        1,
    )
    attn_mixed = (decode_hidden.astype(jnp.float32) + attn_sum).astype(jnp.bfloat16)
    row_count = sequences_local * step_rows
    normed = rms_scale(attn_mixed, moe_gain).astype(jnp.bfloat16).reshape(row_count, model_width)
    chosen = jnp.take(expert_table, token_ids.reshape(row_count))
    device_count = ep_count * rep_count
    slot_total = device_count * CAP
    same_expert = chosen[:, None] == chosen[None, :]
    before = jnp.arange(row_count)[None, :] < jnp.arange(row_count)[:, None]
    slot_rank = jnp.sum((same_expert & before).astype(jnp.int32), axis=1)
    destination = chosen * CAP + slot_rank
    send_pick = (jnp.arange(slot_total, dtype=jnp.int32)[:, None] == destination[None, :]).astype(
        jnp.bfloat16
    )
    outgoing = (
        jnp.dot(send_pick, normed, preferred_element_type=jnp.float32)
        .astype(jnp.bfloat16)
        .reshape(device_count, CAP, model_width)
    )
    served = expert_apply(
        lax.all_to_all(outgoing, ("ep", "rep"), split_axis=0, concat_axis=0, tiled=True),
        gate_weight,
        up_weight,
        down_weight,
    )
    returned = lax.all_to_all(served, ("ep", "rep"), split_axis=0, concat_axis=0, tiled=True)
    moe_out = lax.dot_general(
        send_pick,
        returned.reshape(slot_total, model_width),
        (((0,), (0,)), ((), ())),
        preferred_element_type=jnp.float32,
    )
    layer_out = (
        attn_mixed.astype(jnp.float32) + moe_out.reshape(sequences_local, step_rows, model_width)
    ).astype(jnp.bfloat16)
    return layer_out


BF = jnp.bfloat16
F32 = jnp.float32
MESH = pl.DeviceIdType.MESH
KEY_PAD = 32


def rotary_table(count):
    half = HEAD_DIM // 2
    freq = THETA ** (-2.0 * np.arange(half) / HEAD_DIM)
    angle = np.arange(count)[:, None] * freq[None, :]
    cosine, sine = np.cos(angle), np.sin(angle)
    return np.concatenate([cosine, cosine, -sine, sine], axis=1).astype(np.float32)


def iota(shape, dim):
    return lax.broadcasted_iota(jnp.int32, shape, dim)


def turned(vectors, positions, table):
    count = table.shape[0]
    hot = (iota((positions.shape[0], count), 1) == positions).astype(F32)
    both = jnp.dot(hot, table, precision=lax.Precision.HIGHEST, preferred_element_type=F32)
    return vectors * both[:, :HEAD_DIM] + pltpu.roll(vectors, HEAD_DIM // 2, 1) * both[:, HEAD_DIM:]


def fused_kernel(
    dims,
    tok, lens, rot, ph, dh, q, again, kvw, ow, mgain, gw, uw, dw, table,
    out,
    rot_v, ph_v, hid, q_v, again_v, kvw_v, ow_v, mgain_v, gw_v, uw_v, dw_v, table_v,
    picked, kv_send, kv_land, part_send, part_land, tok_send, tok_land, ret_send, ret_land,
    load_sem, hid_s, hid_r, kv_s, kv_r, part_s, part_r, tok_s, tok_r, ret_s, ret_r, own_sem,
):
    ep_n, rep_n, seqs, steps, chunk, step_rows = dims
    ep = lax.axis_index("ep")
    rep = lax.axis_index("rep")
    devices = ep_n * rep_n
    me = ep * rep_n + rep
    rows = seqs * step_rows
    total_rows = rows * rep_n
    qh = q.shape[1] // HEAD_DIM

    far = [lax.rem(rep + 2, rep_n), rep_n - 1 - rep, rep + 1 - 2 * lax.rem(rep, 2)]
    others = [(lax.rem(ep + e, ep_n), r) for r in far for e in range(ep_n)]
    others += [(lax.rem(ep + e, ep_n), rep) for e in range(1, ep_n)]

    def flat(k):
        return {"ep": others[k - 1][0], "rep": others[k - 1][1]}

    loads = {}
    for n, (name, a, b) in enumerate([
        ("dh", dh, hid.at[rep]), ("ph", ph, ph_v), ("again", again, again_v), ("kvw", kvw, kvw_v),
        ("rot", rot, rot_v), ("q", q, q_v), ("table", table, table_v), ("ow", ow, ow_v),
        ("mgain", mgain, mgain_v), ("gw", gw, gw_v), ("uw", uw, uw_v), ("dw", dw, dw_v),
    ]):
        loads[name] = pltpu.make_async_copy(a, b, load_sem.at[n])
        loads[name].start()

    barrier = pltpu.get_barrier_semaphore()
    for k in range(1, devices):
        pl.semaphore_signal(barrier, inc=1, device_id=flat(k), device_id_type=MESH)
    pl.semaphore_wait(barrier, devices - 1)

    loads["dh"].wait()
    hid_copies = []
    for k in range(1, rep_n):
        peer = far[k - 1]
        c = pltpu.make_async_remote_copy(
            src_ref=hid.at[rep], dst_ref=hid.at[rep], send_sem=hid_s.at[k], recv_sem=hid_r.at[k],
            device_id={"rep": peer}, device_id_type=MESH)
        c.start()
        hid_copies.append(c)

    def normed(values, gain):
        wide = values.astype(F32)
        mean_sq = jnp.mean(wide * wide, axis=-1, keepdims=True)
        return (wide * lax.rsqrt(mean_sq + EPS) * gain).astype(BF)

    for name in ("ph", "again", "kvw", "rot"):
        loads[name].wait()
    rot_t = rot_v[...]
    prompts = ph.shape[0] // chunk
    proj = jnp.dot(normed(ph_v[...], again_v[...]), kvw_v[...], preferred_element_type=F32)
    pos = ep * chunk + lax.rem(iota((prompts * chunk, 1), 0), chunk)
    keys = turned(proj[:, :HEAD_DIM], pos, rot_t)
    pad = jnp.zeros((KEY_PAD - chunk, HEAD_DIM), F32)
    for p in range(prompts):
        cut = slice(p * chunk, (p + 1) * chunk)
        kv_send[p, :, :HEAD_DIM] = jnp.concatenate([keys[cut], pad], axis=0).astype(BF)
        kv_send[p, :, HEAD_DIM:] = jnp.concatenate([proj[cut, HEAD_DIM:], pad], axis=0).astype(BF)
    kv_copies = []
    for k in range(1, ep_n):
        peer = lax.rem(ep + k, ep_n)
        c = pltpu.make_async_remote_copy(
            src_ref=kv_send.at[peer], dst_ref=kv_land.at[ep], send_sem=kv_s.at[k], recv_sem=kv_r.at[k],
            device_id={"ep": peer}, device_id_type=MESH)
        c.start()
        kv_copies.append(c)
    kv_own = pltpu.make_async_copy(kv_send.at[ep], kv_land.at[ep], own_sem.at[0])
    kv_own.start()

    loads["q"].wait()
    r0 = iota((total_rows, 1), 0)
    seq0 = lax.div(lax.rem(r0, rows), step_rows)
    step0 = lax.div(r0, rows) * step_rows + lax.rem(r0, step_rows)
    perm = (iota((total_rows, total_rows), 1) == seq0 * steps + step0).astype(BF)
    q_perm = jnp.dot(perm, q_v[...], preferred_element_type=F32)
    q_cat = jnp.concatenate(
        [q_perm[:, h * HEAD_DIM:(h + 1) * HEAD_DIM] for h in range(qh)], axis=0).astype(BF)

    loads["table"].wait()
    i0 = iota((rows, 1), 0)
    lane = jnp.zeros((rows, 1), jnp.int32)
    for i in range(rows):
        t = tok[i % step_rows, i // step_rows]
        picked[pl.ds(i, 1), :] = table_v[pl.ds(lax.shift_right_logical(t, 7), 1), :]
        lane = jnp.where(i0 == i, t & 127, lane)
    got = picked[...].astype(F32)
    chosen_c = jnp.sum(jnp.where(iota(got.shape, 1) == lane, got, 0.0), axis=1, keepdims=True)
    a_i, b_i = iota((rows, rows), 0), iota((rows, rows), 1)
    chosen_r = jnp.sum(jnp.where(a_i == b_i, chosen_c, 0.0), axis=0, keepdims=True)
    same = chosen_c == chosen_r
    rank_c = jnp.sum(jnp.where(same & (b_i < a_i), 1.0, 0.0), axis=1, keepdims=True)
    rank_r = jnp.sum(jnp.where(same & (a_i < b_i), 1.0, 0.0), axis=0, keepdims=True)
    slots = devices * CAP
    dest_r = (chosen_r * CAP + rank_r).astype(jnp.int32)
    dest_c = (chosen_c * CAP + rank_c).astype(jnp.int32)
    pick = (iota((slots, rows), 0) == dest_r).astype(BF)
    unpick = (iota((rows, slots), 1) == dest_c).astype(BF)

    length = lens[ep]
    keys_p = ep_n * KEY_PAD
    n_keys = keys_p + total_rows
    qr = lax.rem(iota((qh * total_rows, 1), 0), total_rows)
    q_seq = lax.div(lax.rem(qr, rows), step_rows)
    q_step = lax.div(qr, rows) * step_rows + lax.rem(qr, step_rows)
    kc = iota((1, n_keys), 1)
    inner = lax.rem(kc, KEY_PAD)
    p_ok = (kc < keys_p) & (inner < chunk) & (lax.div(kc, KEY_PAD) * chunk + inner < length)
    kr = jnp.maximum(kc - keys_p, 0)
    k_seq = jnp.where(kc < keys_p, -1, lax.div(lax.rem(kr, rows), step_rows))
    k_step = jnp.where(p_ok, -1, lax.div(kr, rows) * step_rows + lax.rem(kr, step_rows))
    k_seq_p = jnp.where(p_ok, 1, 0)
    mask = ((q_seq == k_seq) | (k_seq_p == 1)) & (k_step <= q_step)

    for c in hid_copies:
        c.wait_recv()
    hidden = jnp.concatenate([hid[r, s] for r in range(rep_n) for s in range(seqs)], axis=0)
    proj_d = jnp.dot(normed(hidden, again_v[...]), kvw_v[...], preferred_element_type=F32)
    keys_d = turned(proj_d[:, :HEAD_DIM], length + step0, rot_t).astype(BF)
    vals_d = proj_d[:, HEAD_DIM:].astype(BF)
    for c in kv_copies:
        c.wait_recv()
    kv_own.wait()
    kv_all = kv_land[...].reshape(keys_p, 2 * HEAD_DIM)
    k_all = jnp.concatenate([kv_all[:, :HEAD_DIM], keys_d], axis=0)
    v_all = jnp.concatenate([kv_all[:, HEAD_DIM:], vals_d], axis=0)
    scores = lax.dot_general(
        q_cat, k_all, (((1,), (1,)), ((), ())), preferred_element_type=F32) * HEAD_DIM ** (-0.5)
    scores = jnp.where(mask, scores, -1e30)
    top = jnp.max(scores, axis=-1, keepdims=True)
    weights = jnp.where(mask, jnp.exp(scores - top), 0.0)
    row_total = jnp.sum(weights, axis=-1, keepdims=True)
    att = jnp.dot(weights.astype(BF), v_all, preferred_element_type=F32) / row_total
    att = jnp.concatenate(
        [att[h * total_rows:(h + 1) * total_rows] for h in range(qh)], axis=1).astype(BF)
    loads["ow"].wait()
    part = jnp.dot(att, ow_v[...], preferred_element_type=F32).astype(BF)
    part_send[...] = part.reshape(part_send.shape)
    part_copies = []
    for k in range(1, rep_n):
        peer = far[k - 1]
        c = pltpu.make_async_remote_copy(
            src_ref=part_send.at[peer], dst_ref=part_land.at[k - 1], send_sem=part_s.at[k],
            recv_sem=part_r.at[k], device_id={"rep": peer}, device_id_type=MESH)
        c.start()
        part_copies.append(c)
    attn_sum = part_send[rep].astype(F32)
    loads["mgain"].wait()
    for k, c in enumerate(part_copies):
        c.wait_recv()
        attn_sum = attn_sum + part_land[k].astype(F32)
    own = jnp.concatenate([hid[rep, s] for s in range(seqs)], axis=0)
    mixed = (own.astype(F32) + attn_sum).astype(BF)
    tokens = normed(mixed, mgain_v[...])

    def scatter(values, send, land, sends, recvs, own):
        for d in range(devices):
            send[d] = values[d * CAP:(d + 1) * CAP, :]
        copies = []
        for k in range(1, devices):
            other = others[k - 1][0] * rep_n + others[k - 1][1]
            c = pltpu.make_async_remote_copy(
                src_ref=send.at[other], dst_ref=land.at[me], send_sem=sends.at[k],
                recv_sem=recvs.at[k], device_id=flat(k), device_id_type=MESH)
            c.start()
            copies.append(c)
        mine = pltpu.make_async_copy(send.at[me], land.at[me], own)
        mine.start()
        return copies, mine

    outgoing = jnp.dot(pick, tokens, preferred_element_type=F32).astype(BF)
    tok_copies, tok_own = scatter(outgoing, tok_send, tok_land, tok_s, tok_r, own_sem.at[1])
    for name in ("gw", "uw", "dw"):
        loads[name].wait()
    for c in tok_copies:
        c.wait_recv()
    tok_own.wait()
    served_in = jnp.concatenate([tok_land[d] for d in range(devices)], axis=0)
    gate = jnp.dot(served_in, gw_v[...], preferred_element_type=F32)
    up = jnp.dot(served_in, uw_v[...], preferred_element_type=F32)
    act = (gate / (1.0 + jnp.exp(-gate)) * up).astype(BF)
    served = jnp.dot(act, dw_v[...], preferred_element_type=F32).astype(BF)
    ret_copies, ret_own = scatter(served, ret_send, ret_land, ret_s, ret_r, own_sem.at[2])
    for c in ret_copies:
        c.wait_recv()
    ret_own.wait()
    back = jnp.concatenate([ret_land[d] for d in range(devices)], axis=0)
    moe = jnp.dot(unpick, back, preferred_element_type=F32)
    done = (mixed.astype(F32) + moe).astype(BF)
    for s in range(seqs):
        out[s] = done[s * step_rows:(s + 1) * step_rows, :]
    for c in hid_copies + kv_copies + part_copies + tok_copies + ret_copies:
        c.wait_send()


def fused_local(
    prompt_hidden, decode_hidden, queries, attn_gain, key_value_weight, out_weight, moe_gain,
    gate_weight, up_weight, down_weight, expert_table, token_ids, prompt_lengths,
):
    ep_n, rep_n = lax.axis_size("ep"), lax.axis_size("rep")
    prompts, chunk, width = prompt_hidden.shape
    seqs, step_rows, _ = decode_hidden.shape
    steps = queries.shape[1]
    ff = gate_weight.shape[2]
    devices = ep_n * rep_n
    rows = seqs * step_rows
    columns = key_value_weight.shape[1]
    count = -(-(chunk * ep_n + steps) // 128) * 128
    dims = (ep_n, rep_n, seqs, steps, chunk, step_rows)
    any_spec = pl.BlockSpec(memory_space=pl.ANY)
    smem = pl.BlockSpec(memory_space=pltpu.SMEM)
    vm = pltpu.VMEM
    dma = pltpu.SemaphoreType.DMA
    args = (
        token_ids.T, prompt_lengths, jnp.asarray(rotary_table(count)),
        prompt_hidden.reshape(prompts * chunk, width), decode_hidden,
        queries.reshape(seqs * steps, queries.shape[2]), attn_gain.reshape(1, width),
        key_value_weight, out_weight, moe_gain.reshape(1, width),
        gate_weight[0], up_weight[0], down_weight[0], expert_table.reshape(-1, 128),
    )
    slab = (devices, CAP, width)
    out = pl.pallas_call(
        functools.partial(fused_kernel, dims),
        out_shape=pltpu.VMEM(decode_hidden.shape, BF),
        in_specs=[smem, smem] + [any_spec] * 12,
        out_specs=pl.BlockSpec(memory_space=pltpu.VMEM),
        scratch_shapes=[
            vm((count, 2 * HEAD_DIM), F32), vm((prompts * chunk, width), BF), vm((rep_n,) + decode_hidden.shape, BF),
            vm((seqs * steps, queries.shape[2]), BF), vm((1, width), F32), vm((width, columns), BF),
            vm(out_weight.shape, BF), vm((1, width), F32), vm((width, ff), BF), vm((width, ff), BF),
            vm((ff, width), BF), vm((expert_table.shape[0] // 128, 128), jnp.int32),
            vm((rows, 128), jnp.int32),
            vm((prompts, KEY_PAD, columns), BF), vm((ep_n, KEY_PAD, columns), BF),
            vm((rep_n, rows, width), BF), vm((rep_n - 1, rows, width), BF),
            vm(slab, BF), vm(slab, BF), vm(slab, BF), vm(slab, BF),
            dma((12,)), dma((rep_n,)), dma((rep_n,)), dma((ep_n,)), dma((ep_n,)), dma((rep_n,)),
            dma((rep_n,)), dma((devices,)), dma((devices,)), dma((devices,)), dma((devices,)), dma((3,)),
        ],
        compiler_params=pltpu.CompilerParams(
            collective_id=0, has_side_effects=True, vmem_limit_bytes=60 * 1024 * 1024),
    )(*args)
    return out


def pick_local(*args):
    prompt_hidden, decode_hidden, queries, key_value_weight = args[0], args[1], args[2], args[4]
    one_prompt = (
        decode_hidden.shape[0] * lax.axis_size("ep") // GROUP_PROMPTS == decode_hidden.shape[0]
        and lax.axis_size("ep") == GROUP_PROMPTS
    )
    four = lax.axis_size("rep") == 4
    one_head = key_value_weight.shape[1] == 2 * HEAD_DIM
    if four and one_prompt and one_head and prompt_hidden.shape[1] <= KEY_PAD and prompt_hidden.shape[1] % 8 == 0:
        return fused_local(*args)
    return local(*args)


def solution(mesh):
    placed = (
        P("groups", "ep", None),
        P(("groups", "ep"), "rep", None),
        P(("groups", "ep"), None, "rep"),
        P(),
        P(None, "rep"),
        P("rep", None),
        P(),
        P(("ep", "rep"), None, None),
        P(("ep", "rep"), None, None),
        P(("ep", "rep"), None, None),
        P(),
        P("ep", "rep"),
        P("groups"),
    )
    return jax.shard_map(
        pick_local,
        mesh=mesh,
        in_specs=placed,
        out_specs=P(("groups", "ep"), "rep", None),
        check_vma=False,
    )
```

```python
import math

import functools

import jax
import jax.numpy as jnp
import numpy as np
from jax import lax
from jax.experimental import pallas as pl
from jax.experimental.pallas import tpu as pltpu
from jax.sharding import PartitionSpec as P

HEAD_DIM = 128
QUERY_HEADS = 16
KEY_VALUE_HEADS = 4
GROUP_PROMPTS = 4
CAP = 2


EPS = 1e-06
THETA = 1000000.0


def swapped(block, axis, bit):
    count = lax.axis_size(axis)
    route = []
    for low in range(count):
        high = low | 1 << bit
        if high != low and high < count:
            route += [(low, high), (high, low)]
    return lax.ppermute(block, axis, route)


def rms_scale(hidden, gain_vec):
    widened = hidden.astype(jnp.float32)
    mean_sq = jnp.mean(widened * widened, axis=-1, keepdims=True)
    return widened * lax.rsqrt(mean_sq + EPS) * gain_vec


def rotate(vectors, positions):
    half_dim = vectors.shape[-1] // 2
    inverse_freq = jnp.exp(
        jnp.arange(half_dim, dtype=jnp.float32) * (-2.0 * math.log(THETA) / vectors.shape[-1])
    )
    angles = positions[..., None] * inverse_freq
    cosine = jnp.cos(angles)
    sine_part = jnp.sin(angles)
    first_half = vectors[..., :half_dim]
    second_half = vectors[..., half_dim:]
    return jnp.concatenate(
        [
            first_half * cosine - second_half * sine_part,
            second_half * cosine + first_half * sine_part,
        ],
        axis=-1,
    )


def expert_apply(tokens, gate_weight, up_weight, down_weight):
    flat_rows = tokens.reshape(-1, tokens.shape[-1])
    gate_proj = jnp.dot(flat_rows, gate_weight[0], preferred_element_type=jnp.float32)
    up_proj = jnp.dot(flat_rows, up_weight[0], preferred_element_type=jnp.float32)
    hidden = (jax.nn.silu(gate_proj) * up_proj).astype(jnp.bfloat16)
    return (
        jnp.dot(hidden, down_weight[0], preferred_element_type=jnp.float32)
        .astype(jnp.bfloat16)
        .reshape(tokens.shape)
    )


def local(
    prompt_hidden,
    decode_hidden,
    queries,
    attn_gain,
    key_value_weight,
    out_weight,
    moe_gain,
    gate_weight,
    up_weight,
    down_weight,
    expert_table,
    token_ids,
    prompt_lengths,
):
    full_hidden = lax.all_gather(decode_hidden, "rep", axis=1, tiled=True)
    sequences_local, steps_total, model_width = full_hidden.shape
    prompt_length_local = prompt_hidden.shape[1]
    qh_dev = queries.shape[2] // HEAD_DIM
    group_count = QUERY_HEADS // KEY_VALUE_HEADS
    ep_count = lax.axis_size("ep")
    rep_count = lax.axis_size("rep")
    ep_index = lax.axis_index("ep")
    rep_index = lax.axis_index("rep")
    seq_total = sequences_local * ep_count
    samples = seq_total // GROUP_PROMPTS
    score_scale = HEAD_DIM ** (-0.5)
    step_rows = steps_total // rep_count
    blocks = key_value_weight.shape[1] // HEAD_DIM

    def own_columns(hidden, positions):
        leading = hidden.shape[:-1]
        normed = rms_scale(hidden, attn_gain).astype(jnp.bfloat16)
        projected = jnp.dot(
            normed.reshape(-1, model_width), key_value_weight, preferred_element_type=jnp.float32
        )
        projected = projected.reshape(leading + (blocks, HEAD_DIM))
        block_ids = rep_index * blocks + jnp.arange(blocks, dtype=jnp.int32)
        is_key = (block_ids % 2 == 0)[:, None]
        turned = rotate(projected, positions[..., None])
        return (
            jnp.where(is_key, turned, projected)
            .astype(jnp.bfloat16)
            .reshape(leading + (blocks * HEAD_DIM,))
        )

    key_pos = ep_index * prompt_length_local + jnp.arange(prompt_length_local, dtype=jnp.int32)
    prompt_pos = jnp.broadcast_to(
        key_pos.astype(jnp.float32)[None, :], (GROUP_PROMPTS, prompt_length_local)
    )
    own_seqs = ep_index * sequences_local + jnp.arange(sequences_local, dtype=jnp.int32)
    own_prompt = own_seqs // samples
    own_lengths = jnp.take(prompt_lengths, own_prompt)
    decode_pos = (
        own_lengths[:, None].astype(jnp.float32)
        + jnp.arange(steps_total, dtype=jnp.float32)[None, :]
    )
    prompt_part = own_columns(prompt_hidden, prompt_pos)
    decode_part = own_columns(full_hidden, decode_pos)
    prompt_hot = own_prompt[:, None] == jnp.arange(GROUP_PROMPTS, dtype=jnp.int32)[None, :]
    if blocks == 1:
        partner_prompt, partner_decode = swapped((prompt_part, decode_part), "rep", 0)
        holds_key = rep_index % 2 == 0
        prompt_columns = jnp.where(
            holds_key,
            jnp.concatenate([prompt_part, partner_prompt], axis=2),
            jnp.concatenate([partner_prompt, prompt_part], axis=2),
        )
        decode_columns = jnp.where(
            holds_key,
            jnp.concatenate([decode_part, partner_decode], axis=2),
            jnp.concatenate([partner_decode, decode_part], axis=2),
        )
        heads_here = 1
        head_base = rep_index // 2
    else:
        prompt_columns = prompt_part
        decode_columns = decode_part
        heads_here = blocks // 2
        head_base = rep_index * heads_here
    prompt_key_value = prompt_columns.reshape(
        GROUP_PROMPTS, prompt_length_local, heads_here, 2, HEAD_DIM
    )
    decode_key_value = decode_columns.reshape(sequences_local, steps_total, heads_here, 2, HEAD_DIM)
    prompt_keys = prompt_key_value[:, :, :, 0, :]
    prompt_values = prompt_key_value[:, :, :, 1, :]
    decode_keys = decode_key_value[:, :, :, 0, :]
    decode_values = decode_key_value[:, :, :, 1, :]
    query_matrix = queries.reshape(sequences_local, steps_total, qh_dev, HEAD_DIM)
    head_pick = (
        rep_index * qh_dev + jnp.arange(qh_dev, dtype=jnp.int32)
    ) // group_count - head_base
    own_keys = jnp.take(decode_keys, head_pick, axis=2)
    own_values = jnp.take(decode_values, head_pick, axis=2)
    self_scores = (
        jnp.einsum("sthd,suhd->sthu", query_matrix, own_keys, preferred_element_type=jnp.float32)
        * score_scale
    )
    self_mask = (
        jnp.arange(steps_total, dtype=jnp.int32)[None, :]
        <= jnp.arange(steps_total, dtype=jnp.int32)[:, None]
    )[None, :, None, :]
    self_scores = jnp.where(self_mask, self_scores, -1e30)
    self_top = jnp.max(self_scores, axis=-1)
    start_weights = jnp.where(self_mask, jnp.exp(self_scores - self_top[..., None]), 0.0)
    row_top = self_top
    row_total = jnp.sum(start_weights, axis=-1)
    weighted = jnp.einsum(
        "sthu,suhd->sthd",
        start_weights.astype(jnp.bfloat16),
        own_values,
        preferred_element_type=jnp.float32,
    )
    piece_keys = jnp.take(lax.all_gather(prompt_keys, "ep", axis=1, tiled=True), head_pick, axis=2)
    piece_values = jnp.take(
        lax.all_gather(prompt_values, "ep", axis=1, tiled=True), head_pick, axis=2
    )
    piece_len = piece_keys.shape[1]
    valid = jnp.arange(piece_len, dtype=jnp.int32)[None, :] < prompt_lengths[:, None]
    key_mask = prompt_hot[:, None, None, :, None] & valid[None, None, None, :, :]
    scores = (
        jnp.einsum("sthd,pnhd->sthpn", query_matrix, piece_keys, preferred_element_type=jnp.float32)
        * score_scale
    )
    scores = jnp.where(key_mask, scores, -1e30)
    new_top = jnp.maximum(row_top, jnp.max(scores, axis=(-2, -1)))
    decay = jnp.exp(row_top - new_top)
    weights = jnp.where(key_mask, jnp.exp(scores - new_top[..., None, None]), 0.0)
    weighted = weighted * decay[..., None] + jnp.einsum(
        "sthpn,pnhd->sthd",
        weights.astype(jnp.bfloat16),
        piece_values,
        preferred_element_type=jnp.float32,
    )
    row_top, row_total, weighted = (
        new_top,
        row_total * decay + jnp.sum(weights, axis=(-2, -1)),
        weighted,
    )
    attended = weighted / row_total[..., None]
    heads_out = attended.reshape(sequences_local, steps_total, qh_dev * HEAD_DIM).astype(
        jnp.bfloat16
    )
    by_step = jnp.swapaxes(heads_out, 0, 1)
    attn_sum = jnp.swapaxes(
        lax.psum_scatter(
            jnp.dot(
                by_step.reshape(-1, by_step.shape[-1]),
                out_weight,
                preferred_element_type=jnp.float32,
            )
            .reshape(step_rows * lax.axis_size("rep"), sequences_local, model_width)
            .astype(jnp.bfloat16),
            "rep",
            scatter_dimension=0,
            tiled=True,
        ).astype(jnp.float32),
        0,
        1,
    )
    attn_mixed = (decode_hidden.astype(jnp.float32) + attn_sum).astype(jnp.bfloat16)
    row_count = sequences_local * step_rows
    normed = rms_scale(attn_mixed, moe_gain).astype(jnp.bfloat16).reshape(row_count, model_width)
    chosen = jnp.take(expert_table, token_ids.reshape(row_count))
    device_count = ep_count * rep_count
    slot_total = device_count * CAP
    same_expert = chosen[:, None] == chosen[None, :]
    before = jnp.arange(row_count)[None, :] < jnp.arange(row_count)[:, None]
    slot_rank = jnp.sum((same_expert & before).astype(jnp.int32), axis=1)
    destination = chosen * CAP + slot_rank
    send_pick = (jnp.arange(slot_total, dtype=jnp.int32)[:, None] == destination[None, :]).astype(
        jnp.bfloat16
    )
    outgoing = (
        jnp.dot(send_pick, normed, preferred_element_type=jnp.float32)
        .astype(jnp.bfloat16)
        .reshape(device_count, CAP, model_width)
    )
    served = expert_apply(
        lax.all_to_all(outgoing, ("ep", "rep"), split_axis=0, concat_axis=0, tiled=True),
        gate_weight,
        up_weight,
        down_weight,
    )
    returned = lax.all_to_all(served, ("ep", "rep"), split_axis=0, concat_axis=0, tiled=True)
    moe_out = lax.dot_general(
        send_pick,
        returned.reshape(slot_total, model_width),
        (((0,), (0,)), ((), ())),
        preferred_element_type=jnp.float32,
    )
    layer_out = (
        attn_mixed.astype(jnp.float32) + moe_out.reshape(sequences_local, step_rows, model_width)
    ).astype(jnp.bfloat16)
    return layer_out


BF = jnp.bfloat16
F32 = jnp.float32
MESH = pl.DeviceIdType.MESH
KEY_PAD = 32


def rotary_table(count):
    half = HEAD_DIM // 2
    freq = THETA ** (-2.0 * np.arange(half) / HEAD_DIM)
    angle = np.arange(count)[:, None] * freq[None, :]
    cosine, sine = np.cos(angle), np.sin(angle)
    return np.concatenate([cosine, cosine, -sine, sine], axis=1).astype(np.float32)


def iota(shape, dim):
    return lax.broadcasted_iota(jnp.int32, shape, dim)


def turned(vectors, positions, table):
    count = table.shape[0]
    hot = (iota((positions.shape[0], count), 1) == positions).astype(F32)
    both = jnp.dot(hot, table, precision=lax.Precision.HIGHEST, preferred_element_type=F32)
    return vectors * both[:, :HEAD_DIM] + pltpu.roll(vectors, HEAD_DIM // 2, 1) * both[:, HEAD_DIM:]


def fused_kernel(
    dims,
    tok_in, lens_in, rot, ph, dh, q, again, kvw, ow, mgain, gw, uw, dw, table,
    out,
    tok, lens, rot_v, ph_v, hid, q_v, again_v, kvw_v, ow_v, mgain_v, gw_v, uw_v, dw_v, table_v,
    picked, kv_send, kv_land, part_send, part_land, tok_send, tok_land, ret_send, ret_land,
    load_sem, hid_s, hid_r, kv_s, kv_r, part_s, part_r, tok_s, tok_r, ret_s, ret_r, own_sem,
):
    ep_n, rep_n, seqs, steps, chunk, step_rows = dims
    ep = lax.axis_index("ep")
    rep = lax.axis_index("rep")
    devices = ep_n * rep_n
    me = ep * rep_n + rep
    rows = seqs * step_rows
    total_rows = rows * rep_n
    qh = q.shape[1] // HEAD_DIM

    far = [lax.rem(rep + 2, rep_n), rep_n - 1 - rep, rep + 1 - 2 * lax.rem(rep, 2)]
    others = [(lax.rem(ep + e, ep_n), r) for r in far for e in range(ep_n)]
    others += [(lax.rem(ep + e, ep_n), rep) for e in range(1, ep_n)]

    def flat(k):
        return {"ep": others[k - 1][0], "rep": others[k - 1][1]}

    loads = {}
    for n, (name, a, b) in enumerate([
        ("dh", dh, hid.at[rep]), ("ph", ph, ph_v), ("again", again, again_v), ("kvw", kvw, kvw_v),
        ("rot", rot, rot_v), ("q", q, q_v), ("table", table, table_v), ("ow", ow, ow_v),
        ("mgain", mgain, mgain_v), ("tok", tok_in, tok), ("lens", lens_in, lens), ("gw", gw, gw_v), ("uw", uw, uw_v), ("dw", dw, dw_v),
    ]):
        loads[name] = pltpu.make_async_copy(a, b, load_sem.at[n])
        loads[name].start()

    barrier = pltpu.get_barrier_semaphore()
    for k in range(1, devices):
        pl.semaphore_signal(barrier, inc=1, device_id=flat(k), device_id_type=MESH)
    pl.semaphore_wait(barrier, devices - 1)

    loads["dh"].wait()
    hid_copies = []
    for k in range(1, rep_n):
        peer = far[k - 1]
        c = pltpu.make_async_remote_copy(
            src_ref=hid.at[rep], dst_ref=hid.at[rep], send_sem=hid_s.at[k], recv_sem=hid_r.at[k],
            device_id={"rep": peer}, device_id_type=MESH)
        c.start()
        hid_copies.append(c)

    def normed(values, gain):
        wide = values.astype(F32)
        mean_sq = jnp.mean(wide * wide, axis=-1, keepdims=True)
        return (wide * lax.rsqrt(mean_sq + EPS) * gain).astype(BF)

    for name in ("ph", "again", "kvw", "rot"):
        loads[name].wait()
    rot_t = rot_v[...]
    prompts = ph.shape[0] // chunk
    proj = jnp.dot(normed(ph_v[...], again_v[...]), kvw_v[...], preferred_element_type=F32)
    pos = ep * chunk + lax.rem(iota((prompts * chunk, 1), 0), chunk)
    keys = turned(proj[:, :HEAD_DIM], pos, rot_t)
    pad = jnp.zeros((KEY_PAD - chunk, HEAD_DIM), F32)
    for p in range(prompts):
        cut = slice(p * chunk, (p + 1) * chunk)
        kv_send[p, :, :HEAD_DIM] = jnp.concatenate([keys[cut], pad], axis=0).astype(BF)
        kv_send[p, :, HEAD_DIM:] = jnp.concatenate([proj[cut, HEAD_DIM:], pad], axis=0).astype(BF)
    kv_copies = []
    for k in range(1, ep_n):
        peer = lax.rem(ep + k, ep_n)
        c = pltpu.make_async_remote_copy(
            src_ref=kv_send.at[peer], dst_ref=kv_land.at[ep], send_sem=kv_s.at[k], recv_sem=kv_r.at[k],
            device_id={"ep": peer}, device_id_type=MESH)
        c.start()
        kv_copies.append(c)
    kv_own = pltpu.make_async_copy(kv_send.at[ep], kv_land.at[ep], own_sem.at[0])
    kv_own.start()

    loads["q"].wait()
    r0 = iota((total_rows, 1), 0)
    seq0 = lax.div(lax.rem(r0, rows), step_rows)
    step0 = lax.div(r0, rows) * step_rows + lax.rem(r0, step_rows)
    perm = (iota((total_rows, total_rows), 1) == seq0 * steps + step0).astype(BF)
    q_perm = jnp.dot(perm, q_v[...], preferred_element_type=F32)
    q_cat = jnp.concatenate(
        [q_perm[:, h * HEAD_DIM:(h + 1) * HEAD_DIM] for h in range(qh)], axis=0).astype(BF)

    loads["table"].wait()
    loads["tok"].wait()
    loads["lens"].wait()
    i0 = iota((rows, 1), 0)
    lane = jnp.zeros((rows, 1), jnp.int32)
    for i in range(rows):
        t = tok[i % step_rows, i // step_rows]
        picked[pl.ds(i, 1), :] = table_v[pl.ds(lax.shift_right_logical(t, 7), 1), :]
        lane = jnp.where(i0 == i, t & 127, lane)
    got = picked[...].astype(F32)
    chosen_c = jnp.sum(jnp.where(iota(got.shape, 1) == lane, got, 0.0), axis=1, keepdims=True)
    a_i, b_i = iota((rows, rows), 0), iota((rows, rows), 1)
    chosen_r = jnp.sum(jnp.where(a_i == b_i, chosen_c, 0.0), axis=0, keepdims=True)
    same = chosen_c == chosen_r
    rank_c = jnp.sum(jnp.where(same & (b_i < a_i), 1.0, 0.0), axis=1, keepdims=True)
    rank_r = jnp.sum(jnp.where(same & (a_i < b_i), 1.0, 0.0), axis=0, keepdims=True)
    slots = devices * CAP
    dest_r = (chosen_r * CAP + rank_r).astype(jnp.int32)
    dest_c = (chosen_c * CAP + rank_c).astype(jnp.int32)
    pick = (iota((slots, rows), 0) == dest_r).astype(BF)
    unpick = (iota((rows, slots), 1) == dest_c).astype(BF)

    length = lens[ep]
    keys_p = ep_n * KEY_PAD
    n_keys = keys_p + total_rows
    qr = lax.rem(iota((qh * total_rows, 1), 0), total_rows)
    q_seq = lax.div(lax.rem(qr, rows), step_rows)
    q_step = lax.div(qr, rows) * step_rows + lax.rem(qr, step_rows)
    kc = iota((1, n_keys), 1)
    inner = lax.rem(kc, KEY_PAD)
    p_ok = (kc < keys_p) & (inner < chunk) & (lax.div(kc, KEY_PAD) * chunk + inner < length)
    kr = jnp.maximum(kc - keys_p, 0)
    k_seq = jnp.where(kc < keys_p, -1, lax.div(lax.rem(kr, rows), step_rows))
    k_step = jnp.where(p_ok, -1, lax.div(kr, rows) * step_rows + lax.rem(kr, step_rows))
    k_seq_p = jnp.where(p_ok, 1, 0)
    mask = ((q_seq == k_seq) | (k_seq_p == 1)) & (k_step <= q_step)

    for c in hid_copies:
        c.wait_recv()
    hidden = jnp.concatenate([hid[r, s] for r in range(rep_n) for s in range(seqs)], axis=0)
    proj_d = jnp.dot(normed(hidden, again_v[...]), kvw_v[...], preferred_element_type=F32)
    keys_d = turned(proj_d[:, :HEAD_DIM], length + step0, rot_t).astype(BF)
    vals_d = proj_d[:, HEAD_DIM:].astype(BF)
    for c in kv_copies:
        c.wait_recv()
    kv_own.wait()
    kv_all = kv_land[...].reshape(keys_p, 2 * HEAD_DIM)
    k_all = jnp.concatenate([kv_all[:, :HEAD_DIM], keys_d], axis=0)
    v_all = jnp.concatenate([kv_all[:, HEAD_DIM:], vals_d], axis=0)
    scores = lax.dot_general(
        q_cat, k_all, (((1,), (1,)), ((), ())), preferred_element_type=F32) * HEAD_DIM ** (-0.5)
    scores = jnp.where(mask, scores, -1e30)
    top = jnp.max(scores, axis=-1, keepdims=True)
    weights = jnp.where(mask, jnp.exp(scores - top), 0.0)
    row_total = jnp.sum(weights, axis=-1, keepdims=True)
    att = jnp.dot(weights.astype(BF), v_all, preferred_element_type=F32) / row_total
    att = jnp.concatenate(
        [att[h * total_rows:(h + 1) * total_rows] for h in range(qh)], axis=1).astype(BF)
    loads["ow"].wait()
    part = jnp.dot(att, ow_v[...], preferred_element_type=F32).astype(BF)
    part_send[...] = part.reshape(part_send.shape)
    part_copies = []
    for k in range(1, rep_n):
        peer = far[k - 1]
        c = pltpu.make_async_remote_copy(
            src_ref=part_send.at[peer], dst_ref=part_land.at[k - 1], send_sem=part_s.at[k],
            recv_sem=part_r.at[k], device_id={"rep": peer}, device_id_type=MESH)
        c.start()
        part_copies.append(c)
    attn_sum = part_send[rep].astype(F32)
    loads["mgain"].wait()
    for k, c in enumerate(part_copies):
        c.wait_recv()
        attn_sum = attn_sum + part_land[k].astype(F32)
    own = jnp.concatenate([hid[rep, s] for s in range(seqs)], axis=0)
    mixed = (own.astype(F32) + attn_sum).astype(BF)
    tokens = normed(mixed, mgain_v[...])

    def scatter(values, send, land, sends, recvs, own):
        for d in range(devices):
            send[d] = values[d * CAP:(d + 1) * CAP, :]
        copies = []
        for k in range(1, devices):
            other = others[k - 1][0] * rep_n + others[k - 1][1]
            c = pltpu.make_async_remote_copy(
                src_ref=send.at[other], dst_ref=land.at[me], send_sem=sends.at[k],
                recv_sem=recvs.at[k], device_id=flat(k), device_id_type=MESH)
            c.start()
            copies.append(c)
        mine = pltpu.make_async_copy(send.at[me], land.at[me], own)
        mine.start()
        return copies, mine

    outgoing = jnp.dot(pick, tokens, preferred_element_type=F32).astype(BF)
    tok_copies, tok_own = scatter(outgoing, tok_send, tok_land, tok_s, tok_r, own_sem.at[1])
    for name in ("gw", "uw", "dw"):
        loads[name].wait()
    for c in tok_copies:
        c.wait_recv()
    tok_own.wait()
    served_in = jnp.concatenate([tok_land[d] for d in range(devices)], axis=0)
    gate = jnp.dot(served_in, gw_v[...], preferred_element_type=F32)
    up = jnp.dot(served_in, uw_v[...], preferred_element_type=F32)
    act = (gate / (1.0 + jnp.exp(-gate)) * up).astype(BF)
    served = jnp.dot(act, dw_v[...], preferred_element_type=F32).astype(BF)
    ret_copies, ret_own = scatter(served, ret_send, ret_land, ret_s, ret_r, own_sem.at[2])
    for c in ret_copies:
        c.wait_recv()
    ret_own.wait()
    back = jnp.concatenate([ret_land[d] for d in range(devices)], axis=0)
    moe = jnp.dot(unpick, back, preferred_element_type=F32)
    done = (mixed.astype(F32) + moe).astype(BF)
    for s in range(seqs):
        out[s] = done[s * step_rows:(s + 1) * step_rows, :]
    for c in hid_copies + kv_copies + part_copies + tok_copies + ret_copies:
        c.wait_send()


def fused_local(
    prompt_hidden, decode_hidden, queries, attn_gain, key_value_weight, out_weight, moe_gain,
    gate_weight, up_weight, down_weight, expert_table, token_ids, prompt_lengths,
):
    ep_n, rep_n = lax.axis_size("ep"), lax.axis_size("rep")
    prompts, chunk, width = prompt_hidden.shape
    seqs, step_rows, _ = decode_hidden.shape
    steps = queries.shape[1]
    ff = gate_weight.shape[2]
    devices = ep_n * rep_n
    rows = seqs * step_rows
    columns = key_value_weight.shape[1]
    count = -(-(chunk * ep_n + steps) // 128) * 128
    dims = (ep_n, rep_n, seqs, steps, chunk, step_rows)
    any_spec = pl.BlockSpec(memory_space=pl.ANY)
    vm = pltpu.VMEM
    dma = pltpu.SemaphoreType.DMA
    args = (
        token_ids.T, prompt_lengths, jnp.asarray(rotary_table(count)),
        prompt_hidden.reshape(prompts * chunk, width), decode_hidden,
        queries.reshape(seqs * steps, queries.shape[2]), attn_gain.reshape(1, width),
        key_value_weight, out_weight, moe_gain.reshape(1, width),
        gate_weight[0], up_weight[0], down_weight[0], expert_table.reshape(-1, 128),
    )
    slab = (devices, CAP, width)
    out = pl.pallas_call(
        functools.partial(fused_kernel, dims),
        out_shape=pltpu.VMEM(decode_hidden.shape, BF),
        in_specs=[any_spec] * 14,
        out_specs=pl.BlockSpec(memory_space=pltpu.VMEM),
        scratch_shapes=[
            pltpu.SMEM((step_rows, seqs), jnp.int32), pltpu.SMEM(prompt_lengths.shape, jnp.int32),
            vm((count, 2 * HEAD_DIM), F32), vm((prompts * chunk, width), BF), vm((rep_n,) + decode_hidden.shape, BF),
            vm((seqs * steps, queries.shape[2]), BF), vm((1, width), F32), vm((width, columns), BF),
            vm(out_weight.shape, BF), vm((1, width), F32), vm((width, ff), BF), vm((width, ff), BF),
            vm((ff, width), BF), vm((expert_table.shape[0] // 128, 128), jnp.int32),
            vm((rows, 128), jnp.int32),
            vm((prompts, KEY_PAD, columns), BF), vm((ep_n, KEY_PAD, columns), BF),
            vm((rep_n, rows, width), BF), vm((rep_n - 1, rows, width), BF),
            vm(slab, BF), vm(slab, BF), vm(slab, BF), vm(slab, BF),
            dma((14,)), dma((rep_n,)), dma((rep_n,)), dma((ep_n,)), dma((ep_n,)), dma((rep_n,)),
            dma((rep_n,)), dma((devices,)), dma((devices,)), dma((devices,)), dma((devices,)), dma((3,)),
        ],
        compiler_params=pltpu.CompilerParams(
            collective_id=0, has_side_effects=True, vmem_limit_bytes=60 * 1024 * 1024),
    )(*args)
    return out


def pick_local(*args):
    prompt_hidden, decode_hidden, queries, key_value_weight = args[0], args[1], args[2], args[4]
    one_prompt = (
        decode_hidden.shape[0] * lax.axis_size("ep") // GROUP_PROMPTS == decode_hidden.shape[0]
        and lax.axis_size("ep") == GROUP_PROMPTS
    )
    four = lax.axis_size("rep") == 4
    one_head = key_value_weight.shape[1] == 2 * HEAD_DIM
    if four and one_prompt and one_head and prompt_hidden.shape[1] <= KEY_PAD and prompt_hidden.shape[1] % 8 == 0:
        return fused_local(*args)
    return local(*args)


def solution(mesh):
    placed = (
        P("groups", "ep", None),
        P(("groups", "ep"), "rep", None),
        P(("groups", "ep"), None, "rep"),
        P(),
        P(None, "rep"),
        P("rep", None),
        P(),
        P(("ep", "rep"), None, None),
        P(("ep", "rep"), None, None),
        P(("ep", "rep"), None, None),
        P(),
        P("ep", "rep"),
        P("groups"),
    )
    return jax.shard_map(
        pick_local,
        mesh=mesh,
        in_specs=placed,
        out_specs=P(("groups", "ep"), "rep", None),
        check_vma=False,
    )
```
